32 devices in a mesh: gx: 8 (over y, x, core), gy: 4 (over z).
Axes of the slice: x: 2, y: 2, z: 4, core: 2. Of those that a mesh axis runs over, the one named last changes fastest.
Arguments:
- activations: bfloat16 [40960, 5120], P(('gx', 'gy')), may hold values from -6 to 6
- out_grad: bfloat16 [2, 40960, 32], P(None, ('gx', 'gy')), may hold values from -0.0390625 to 0.0390625
- master: float32 [32, 2, 5120], P(('gx', 'gy')), may hold values from -1 to 1
- first_moment: bfloat16 [32, 2, 5120], P(('gx', 'gy')), may hold values from -1 to 1
- first_scale: float32 [32, 2, 40], P(('gx', 'gy')), may hold values from 0.05 to 0.5
- second_moment: bfloat16 [32, 2, 5120], P(('gx', 'gy')), may hold values from 0.099609375 to 1
- second_scale: float32 [32, 2, 40], P(('gx', 'gy')), may hold values from 0.05 to 0.5
Outputs:
- new_weights: bfloat16 [32, 2, 5120], replicated
- new_master: float32 [32, 2, 5120], P(('gx', 'gy'))
- new_first: bfloat16 [32, 2, 5120], P(('gx', 'gy'))
- new_first_scale: float32 [32, 2, 40], P(('gx', 'gy'))
- new_second: bfloat16 [32, 2, 5120], P(('gx', 'gy'))
- new_second_scale: float32 [32, 2, 40], P(('gx', 'gy'))
The draws below stay inside these ranges and needn't reach their ends.
All inputs are finite; a program needn't handle non-finite values. Where the reference program divides by a largest or mean magnitude, that divisor is 1e-20 or more.
Results may differ from the reference program's by a relative error of at most 0.0014.
Values may be sent and summed in bfloat16 or wider, within the bound.
A program may use at most 128 MiB of HBM per device.

```python
import math
import jax
import jax.numpy as jnp
from jax import lax

D = 5120
GROUP = 128
TOKENS = 40960
ROWS = 32


def with_spikes(array, rng, source, target, parts, factor):
    owner, partner = [(jnp.arange(array.shape[dim]) // (array.shape[dim] // parts)).reshape([-1 if axis == dim else 1 for axis in range(array.ndim)]) for dim in (source, target)]
    chosen = jax.random.permutation(rng, parts)[partner]
    strong = (owner == chosen) | (owner == (partner + parts // 2) % parts)
    return jnp.where(strong, factor * array, array)


def block_levels(stream_key, shape, cuts, smallest, largest):
    def one(position, parts):
        steps = jax.random.uniform(jax.random.fold_in(jax.random.fold_in(stream_key, 6), position), (parts,), jnp.float32, smallest / len(cuts), largest / len(cuts))
        return jnp.repeat(jnp.exp(steps), shape[position] // parts).reshape((-1,) + (1,) * (len(shape) - position - 1))

    loudness = one(*cuts[0])
    for cut in cuts[1:]:
        loudness = loudness * one(*cut)
    return loudness


def noise(key, shape, spread, reach, shards=(), held_as=jnp.bfloat16):
    entries = jax.random.normal(key, shape, jnp.float32) * spread
    if len(shards) > 0:
        entries = block_levels(key, shape, shards, -0.22, 0.18) * entries
    return jnp.clip(entries, min=-reach, max=reach).astype(held_as)


def gaussian_with(own_key, shape, spread, bound, pieces, heavy, dtype=jnp.bfloat16):
    drawn = spread * jax.random.normal(own_key, shape, jnp.float32)
    if pieces:
        drawn = drawn * block_levels(own_key, shape, pieces, -0.22, 0.18)
    return jnp.clip(with_spikes(drawn, jax.random.fold_in(own_key, 3), *heavy), -bound, bound).astype(dtype)


def setup_inputs(seed: int = 0) -> dict:
    arg_keys = jax.random.split(jax.random.key(seed), 8)
    activations = noise(arg_keys[0], (TOKENS, D), 1.0, 6.0, ((0, 32),))
    out_grad = gaussian_with(arg_keys[1], (2, TOKENS, ROWS), (0.3 / TOKENS ** 0.5), 0.0390625, ((1, 32),), (1, 2, 32, 2.75))
    master = jnp.clip(jax.random.uniform(arg_keys[2], (ROWS, 2, D), jnp.float32, -1.0, 1.0) * block_levels(arg_keys[2], (ROWS, 2, D), ((0, 32),), -0.4, 0.0), -1.0, 1.0)
    first_moment = jnp.clip(jax.random.uniform(arg_keys[3], (ROWS, 2, D), jnp.float32, -1.0, 1.0) * block_levels(arg_keys[3], (ROWS, 2, D), ((0, 32),), -0.4, 0.0), -1.0, 1.0).astype(jnp.bfloat16)
    first_scale = jnp.clip(jnp.exp(math.log(0.5) - 2.3025851 * jax.random.uniform(arg_keys[4], (ROWS, 2, D // GROUP), jnp.float32) ** block_levels(arg_keys[4], (ROWS, 2, D // GROUP), ((0, 32),), -0.2, 0.2)), 0.05, 0.5)
    second_moment = jnp.clip(0.099609375 + 0.9003906 * jax.random.uniform(arg_keys[5], (ROWS, 2, D), jnp.float32) ** block_levels(arg_keys[5], (ROWS, 2, D), ((0, 32),), -0.2, 0.2), 0.099609375, 1.0).astype(jnp.bfloat16)
    second_scale = jnp.clip(jnp.exp(math.log(0.5) - 2.3025851 * jax.random.uniform(arg_keys[6], (ROWS, 2, D // GROUP), jnp.float32) ** block_levels(arg_keys[6], (ROWS, 2, D // GROUP), ((0, 32),), -0.2, 0.2)), 0.05, 0.5)
    return {"activations": activations, "out_grad": out_grad, "master": master, "first_moment": first_moment, "first_scale": first_scale, "second_moment": second_moment, "second_scale": second_scale}


beta_one = 0.9
beta_two = 0.95
epsilon = 1e-08
learn_rate = 0.01
decay_rate = 0.1
step_count = 10

def expand(quant, scales):
    row_count, pair_count, width_all = quant.shape
    group_count = scales.shape[2]
    blocks = quant.astype(jnp.float32).reshape(row_count, pair_count, group_count, width_all // group_count)
    return (blocks * scales[..., None]).reshape(row_count, pair_count, width_all)

def requant(values, group_count):
    row_count, pair_count, width_all = values.shape
    blocks = values.reshape(row_count, pair_count, group_count, width_all // group_count)
    scales = lax.optimization_barrier(jnp.max(jnp.abs(blocks), axis=3)) + 1e-06
    quant = (blocks / scales[..., None]).reshape(row_count, pair_count, width_all).astype(jnp.bfloat16)
    return (quant, scales)

def adam_owned(gradient, master, first_moment, first_scale, second_moment, second_scale):
    group_count = first_scale.shape[2]
    first_old = expand(first_moment, first_scale)
    second_old = expand(second_moment, second_scale)
    first_new = beta_one * first_old + (1.0 - beta_one) * gradient
    second_new = beta_two * second_old + (1.0 - beta_two) * gradient * gradient
    correct_one = 1.0 - beta_one ** step_count
    correct_two = 1.0 - beta_two ** step_count
    update = first_new / correct_one / (jnp.sqrt(second_new / correct_two) + epsilon)
    new_master = master - learn_rate * (update + decay_rate * master)
    new_first, new_first_scale = requant(first_new, group_count)
    new_second, new_second_scale = requant(second_new, group_count)
    return (new_master, new_first, new_first_scale, new_second, new_second_scale)

def reference(activations, out_grad, master, first_moment, first_scale, second_moment, second_scale):
    gate_grad = jnp.dot(out_grad[0].T, activations, preferred_element_type=jnp.float32)
    up_grad = jnp.dot(out_grad[1].T, activations, preferred_element_type=jnp.float32)
    gradient = jnp.stack([gate_grad, up_grad], axis=1)
    new_master, new_first, new_first_scale, new_second, new_second_scale = adam_owned(gradient, master, first_moment, first_scale, second_moment, second_scale)
    new_weights = new_master.astype(jnp.bfloat16)
    return (new_weights, new_master, new_first, new_first_scale, new_second, new_second_scale)
```

```python
import functools

import jax
import jax.numpy as jnp
import numpy as np
from jax import lax
from jax.experimental import pallas as pl
from jax.experimental.pallas import tpu as pltpu
from jax.sharding import PartitionSpec as P

beta_one = 0.9
beta_two = 0.95
epsilon = 1e-08
learn_rate = 0.01
decay_rate = 0.1
step_count = 10

MESH = pl.DeviceIdType.MESH
CHUNKS = 5


def chunk_widths(width_all, group):
    groups = width_all // group
    edges = [groups * i // CHUNKS for i in range(CHUNKS + 1)]
    return [(b - a) * group for a, b in zip(edges, edges[1:])]


def stage_order(count):
    gaps = [0.0, 2.0, 4.0, 3.5, 3.0, 3.5, 1.5]
    items = []
    for c in range(count):
        t = 3.0 + 1.3 * c
        for s, gap in enumerate(gaps):
            t += gap
            items.append((t, s, c))
    return [(s, c) for _, s, c in sorted(items)]


def kernel(nx, ny, widths, group, *refs):
    (act_hbm, og_ref, perm_ref, master_ref, first_ref, fscale_ref, second_ref, sscale_ref,
     w_out, master_out, first_out, fscale_out, second_out, sscale_out) = refs[:14]
    refs = refs[14:]
    n = len(widths)
    lhs, refs = refs[0], refs[1:]
    act, part, rx1, rx2, s2, rx3 = (refs[i * n:(i + 1) * n] for i in range(6))
    (act_sem, p_send, p_recv, q_send, q_recv, g_send, g_recv,
     ag_send, ag_recv, aq_send, aq_recv, ap_send, ap_recv) = refs[6 * n:]
    starts = [sum(widths[:c]) for c in range(n)]

    gx, gy = lax.axis_index("gx"), lax.axis_index("gy")
    nq = nx // 2
    core, quad = lax.rem(gx, 2), gx // 2
    other = 1 - core
    partner = (quad * 2 + other, gy)

    def quad_at(j):
        return lax.rem(quad + j, nq)

    def quad_dev(j):
        return (quad_at(j) * 2 + core, gy)

    def gy_at(j):
        return lax.rem(gy + j, ny)

    def fetch(c):
        return pltpu.make_async_copy(
            act_hbm.at[:, pl.ds(starts[c], widths[c])], act[c], act_sem.at[c])

    for c in range(n):
        fetch(c).start()

    barrier = pltpu.get_barrier_semaphore()
    pl.semaphore_signal(barrier, inc=1, device_id=partner, device_id_type=MESH)
    for j in range(1, nq):
        pl.semaphore_signal(barrier, inc=1, device_id=quad_dev(j), device_id_type=MESH)
    for j in range(1, ny):
        pl.semaphore_signal(barrier, inc=1, device_id=(gx, gy_at(j)), device_id_type=MESH)

    nt = (((1,), (1,)), ((), ()))
    lhs[...] = (
        lax.dot_general(perm_ref[0], og_ref[0], nt, preferred_element_type=jnp.float32)
        + lax.dot_general(perm_ref[1], og_ref[1], nt, preferred_element_type=jnp.float32)
    ).astype(jnp.bfloat16)

    pl.semaphore_wait(barrier, nq + ny - 1)

    def remote(src, dst, send, recv, device):
        return pltpu.make_async_remote_copy(
            src_ref=src, dst_ref=dst, send_sem=send, recv_sem=recv,
            device_id=device, device_id_type=MESH)

    def pair_copy(c):
        return remote(part[c].at[other], rx1[c], p_send.at[c], p_recv.at[c], partner)

    def quad_copy(c, j):
        return remote(part[c].at[core, quad_at(j)], rx2[c].at[j - 1],
                      q_send.at[c, j - 1], q_recv.at[c, j - 1], quad_dev(j))

    def gy_copy(c, j):
        return remote(s2[c].at[gy_at(j)], rx3[c].at[j - 1],
                      g_send.at[c, j - 1], g_recv.at[c, j - 1], (gx, gy_at(j)))

    def rows_of(c, first, count):
        ref = w_out.at[pl.ds(first, count), :, pl.ds(starts[c], widths[c])]
        return ref

    def ag_copy(c, j):
        ref = rows_of(c, gx * ny + gy, 1)
        return remote(ref, ref, ag_send.at[c, j - 1], ag_recv.at[c, j - 1], (gx, gy_at(j)))

    def aq_copy(c, j):
        ref = rows_of(c, gx * ny, ny)
        return remote(ref, ref, aq_send.at[c, j - 1], aq_recv.at[c, j - 1], quad_dev(j))

    def ap_copy(c, j):
        ref = rows_of(c, (quad_at(nq - j) * 2 + core) * ny, ny)
        return remote(ref, ref, ap_send.at[c, j], ap_recv.at[c, j], partner)

    def adam(c, grad):
        gpc = widths[c] // group
        g0 = starts[c] // group
        lane = lax.broadcasted_iota(jnp.int32, (2, fscale_ref.shape[2]), 1)
        fs_all, ss_all = fscale_out[0], sscale_out[0]
        for i in range(gpc):
            cols = pl.ds(starts[c] + i * group, group)
            g = grad[:, i * group:(i + 1) * group]
            fs = fscale_ref[0, :, pl.ds(g0 + i, 1)]
            ss = sscale_ref[0, :, pl.ds(g0 + i, 1)]
            master = master_ref[0, :, cols]
            m_old = first_ref[0, :, cols].astype(jnp.float32) * fs
            v_old = second_ref[0, :, cols].astype(jnp.float32) * ss
            m = beta_one * m_old + (1.0 - beta_one) * g
            v = beta_two * v_old + (1.0 - beta_two) * g * g
            update = m / (1.0 - beta_one**step_count) / (
                jnp.sqrt(v / (1.0 - beta_two**step_count)) + epsilon)
            new = master - learn_rate * (update + decay_rate * master)
            master_out[0, :, cols] = new
            w_out[pl.ds(gx * ny + gy, 1), :, cols] = new.astype(jnp.bfloat16)[None]
            nfs = jnp.max(jnp.abs(m), axis=1, keepdims=True) + 1e-06
            nss = jnp.max(jnp.abs(v), axis=1, keepdims=True) + 1e-06
            first_out[0, :, cols] = (m / nfs).astype(jnp.bfloat16)
            second_out[0, :, cols] = (v / nss).astype(jnp.bfloat16)
            fs_all = jnp.where(lane == g0 + i, nfs, fs_all)
            ss_all = jnp.where(lane == g0 + i, nss, ss_all)
        fscale_out[0], sscale_out[0] = fs_all, ss_all

    fscale_out[...] = jnp.zeros_like(fscale_out)
    sscale_out[...] = jnp.zeros_like(sscale_out)

    for stage, c in stage_order(n):
        if stage == 0:
            fetch(c).wait()
            res = jnp.dot(lhs[...], act[c][...], preferred_element_type=jnp.float32)
            part[c][...] = res.reshape(part[c].shape)
            pair_copy(c).start()
        elif stage == 1:
            pair_copy(c).wait_recv()
            for j in list(range(1, nq)) + [nq]:
                at = quad_at(j)
                part[c][core, at] = part[c][core, at] + rx1[c][at]
                if j < nq:
                    quad_copy(c, j).start()
        elif stage == 2:
            total = part[c][core, quad]
            for j in range(1, nq):
                quad_copy(c, j).wait_recv()
                total = total + rx2[c][j - 1]
            for g in range(ny):
                s2[c][g] = total[2 * g:2 * g + 2]
            for j in range(1, ny):
                gy_copy(c, j).start()
        elif stage == 3:
            grad = s2[c][gy]
            for j in range(1, ny):
                gy_copy(c, j).wait_recv()
                grad = grad + rx3[c][j - 1]
            adam(c, grad)
            for j in range(1, ny):
                ag_copy(c, j).start()
        elif stage == 4:
            for j in range(1, ny):
                ag_copy(c, j).wait_recv()
            for j in range(1, nq):
                aq_copy(c, j).start()
            ap_copy(c, 0).start()
        elif stage == 5:
            for j in range(1, nq):
                aq_copy(c, j).wait_recv()
                ap_copy(c, j).start()
        else:
            for j in range(nq):
                ap_copy(c, j).wait_recv()

    for c in range(n):
        pair_copy(c).wait_send()
        for j in range(1, nq):
            quad_copy(c, j).wait_send()
            aq_copy(c, j).wait_send()
        for j in range(1, ny):
            gy_copy(c, j).wait_send()
            ag_copy(c, j).wait_send()
        for j in range(nq):
            ap_copy(c, j).wait_send()


def body(nx, ny, activations, out_grad, master, first_moment, first_scale, second_moment, second_scale):
    tokens, width_all = activations.shape
    rows = out_grad.shape[2]
    group = width_all // first_scale.shape[2]
    widths = chunk_widths(width_all, group)
    n = len(widths)
    nq = nx // 2
    assert rows == nx * ny and nx % 2 == 0

    perm = np.zeros((2, 2 * rows, rows), np.float32)
    spot = 0
    for core in range(2):
        for quad in range(nq):
            for g in range(ny):
                for p in range(2):
                    perm[p, spot, (quad * 2 + core) * ny + g] = 1.0
                    spot += 1
    perm = jnp.asarray(perm, jnp.bfloat16)

    vmem = pl.BlockSpec(memory_space=pltpu.VMEM)
    f32, bf16 = jnp.float32, jnp.bfloat16
    dma = pltpu.SemaphoreType.DMA
    scratch = [pltpu.VMEM((2 * rows, tokens), bf16)]
    scratch += [pltpu.VMEM((tokens, w), bf16) for w in widths]
    scratch += [pltpu.VMEM((2, nq, 2 * ny, w), f32) for w in widths]
    scratch += [pltpu.VMEM((nq, 2 * ny, w), f32) for w in widths]
    scratch += [pltpu.VMEM((nq - 1, 2 * ny, w), f32) for w in widths]
    scratch += [pltpu.VMEM((ny, 2, w), f32) for w in widths]
    scratch += [pltpu.VMEM((ny - 1, 2, w), f32) for w in widths]
    scratch += [dma((n,)), dma((n,)), dma((n,))]
    scratch += [dma((n, nq - 1)), dma((n, nq - 1)), dma((n, ny - 1)), dma((n, ny - 1))]
    scratch += [dma((n, ny - 1)), dma((n, ny - 1)), dma((n, nq - 1)), dma((n, nq - 1))]
    scratch += [dma((n, nq)), dma((n, nq))]
    shape = jax.ShapeDtypeStruct
    return pl.pallas_call(
        functools.partial(kernel, nx, ny, widths, group),
        out_shape=(
            shape((rows, 2, width_all), bf16),
            shape(master.shape, f32),
            shape(first_moment.shape, bf16),
            shape(first_scale.shape, f32),
            shape(second_moment.shape, bf16),
            shape(second_scale.shape, f32),
        ),
        in_specs=[pl.BlockSpec(memory_space=pl.ANY)] + [vmem] * 7,
        out_specs=[vmem] * 6,
        scratch_shapes=scratch,
        compiler_params=pltpu.CompilerParams(
            collective_id=0, has_side_effects=True, vmem_limit_bytes=60 * 1024 * 1024),
    )(activations, out_grad, perm, master, first_moment, first_scale, second_moment, second_scale)


def solution(mesh):
    nx, ny = mesh.shape["gx"], mesh.shape["gy"]
    rows = P(("gx", "gy"), None, None)
    in_specs = (P(("gx", "gy"), None), P(None, ("gx", "gy"), None), rows, rows, rows, rows, rows)
    out_specs = (P(), rows, rows, rows, rows, rows)
    return jax.shard_map(
        functools.partial(body, nx, ny), mesh=mesh, in_specs=in_specs, out_specs=out_specs,
        check_vma=False)
```

```python
import functools

import jax
import jax.numpy as jnp
import numpy as np
from jax import lax
from jax.experimental import pallas as pl
from jax.experimental.pallas import tpu as pltpu
from jax.sharding import PartitionSpec as P

beta_one = 0.9
beta_two = 0.95
epsilon = 1e-08
learn_rate = 0.01
decay_rate = 0.1
step_count = 10

MESH = pl.DeviceIdType.MESH
CHUNKS = 5


def chunk_widths(width_all, group):
    groups = width_all // group
    edges = [groups * i // CHUNKS for i in range(CHUNKS + 1)]
    return [(b - a) * group for a, b in zip(edges, edges[1:])]


def stage_order(count):
    gaps = [0.0, 2.0, 4.0, 3.5, 3.0, 3.5, 1.5]
    items = []
    for c in range(count):
        t = 3.0 + 1.3 * c
        for s, gap in enumerate(gaps):
            t += gap
            items.append((t, s, c))
    return [(s, c) for _, s, c in sorted(items)]


def kernel(nx, ny, widths, group, *refs):
    act_hbm, held = refs[0], refs[1:8]
    w_out, master_out, first_out, fscale_out, second_out, sscale_out = refs[8:14]
    local = refs[14:21]
    og_ref, perm_ref, master_ref, first_ref, fscale_ref, second_ref, sscale_ref = local
    in_sem = refs[21]
    refs = refs[22:]
    n = len(widths)
    lhs, refs = refs[0], refs[1:]
    act, part, rx1, rx2, s2, rx3 = (refs[i * n:(i + 1) * n] for i in range(6))
    (act_sem, p_send, p_recv, q_send, q_recv, g_send, g_recv,
     ag_send, ag_recv, aq_send, aq_recv, ap_send, ap_recv) = refs[6 * n:]
    starts = [sum(widths[:c]) for c in range(n)]

    gx, gy = lax.axis_index("gx"), lax.axis_index("gy")
    nq = nx // 2
    core, quad = lax.rem(gx, 2), gx // 2
    other = 1 - core
    partner = (quad * 2 + other, gy)

    def quad_at(j):
        return lax.rem(quad + j, nq)

    def quad_dev(j):
        return (quad_at(j) * 2 + core, gy)

    def gy_at(j):
        return lax.rem(gy + j, ny)

    def fetch(c):
        return pltpu.make_async_copy(
            act_hbm.at[:, pl.ds(starts[c], widths[c])], act[c], act_sem.at[c])

    def take(i):
        return pltpu.make_async_copy(held[i], local[i], in_sem.at[i])

    take(0).start()
    take(1).start()
    for c in range(min(2, n)):
        fetch(c).start()
    for i in range(2, 7):
        take(i).start()

    barrier = pltpu.get_barrier_semaphore()
    pl.semaphore_signal(barrier, inc=1, device_id=partner, device_id_type=MESH)
    for j in range(1, nq):
        pl.semaphore_signal(barrier, inc=1, device_id=quad_dev(j), device_id_type=MESH)
    for j in range(1, ny):
        pl.semaphore_signal(barrier, inc=1, device_id=(gx, gy_at(j)), device_id_type=MESH)

    take(0).wait()
    take(1).wait()
    lhs[...] = (
        jnp.dot(perm_ref[0], og_ref[0], preferred_element_type=jnp.float32)
        + jnp.dot(perm_ref[1], og_ref[1], preferred_element_type=jnp.float32)
    ).astype(jnp.bfloat16)

    pl.semaphore_wait(barrier, nq + ny - 1)

    def remote(src, dst, send, recv, device):
        return pltpu.make_async_remote_copy(
            src_ref=src, dst_ref=dst, send_sem=send, recv_sem=recv,
            device_id=device, device_id_type=MESH)

    def pair_copy(c):
        return remote(part[c].at[other], rx1[c], p_send.at[c], p_recv.at[c], partner)

    def quad_copy(c, j):
        return remote(part[c].at[core, quad_at(j)], rx2[c].at[j - 1],
                      q_send.at[c, j - 1], q_recv.at[c, j - 1], quad_dev(j))

    def gy_copy(c, j):
        return remote(s2[c].at[gy_at(j)], rx3[c].at[j - 1],
                      g_send.at[c, j - 1], g_recv.at[c, j - 1], (gx, gy_at(j)))

    def rows_of(c, first, count):
        ref = w_out.at[pl.ds(first, count), :, pl.ds(starts[c], widths[c])]
        return ref

    def ag_copy(c, j):
        ref = rows_of(c, gx * ny + gy, 1)
        return remote(ref, ref, ag_send.at[c, j - 1], ag_recv.at[c, j - 1], (gx, gy_at(j)))

    def aq_copy(c, j):
        ref = rows_of(c, gx * ny, ny)
        return remote(ref, ref, aq_send.at[c, j - 1], aq_recv.at[c, j - 1], quad_dev(j))

    def ap_copy(c, j):
        ref = rows_of(c, (quad_at(nq - j) * 2 + core) * ny, ny)
        return remote(ref, ref, ap_send.at[c, j], ap_recv.at[c, j], partner)

    def adam(c, grad):
        moments = []
        g0 = starts[c] // group
        for i in range(widths[c] // group):
            cols = pl.ds(starts[c] + i * group, group)
            g = grad[:, i * group:(i + 1) * group]
            fs = fscale_ref[0, :, pl.ds(g0 + i, 1)]
            ss = sscale_ref[0, :, pl.ds(g0 + i, 1)]
            master = master_ref[0, :, cols]
            m_old = first_ref[0, :, cols].astype(jnp.float32) * fs
            v_old = second_ref[0, :, cols].astype(jnp.float32) * ss
            m = beta_one * m_old + (1.0 - beta_one) * g
            v = beta_two * v_old + (1.0 - beta_two) * g * g
            update = m / (1.0 - beta_one**step_count) / (
                jnp.sqrt(v / (1.0 - beta_two**step_count)) + epsilon)
            new = master - learn_rate * (update + decay_rate * master)
            master_out[0, :, cols] = new
            w_out[pl.ds(gx * ny + gy, 1), :, cols] = new.astype(jnp.bfloat16)[None]
            moments.append((m, v))
        return moments

    def requant(c, moments):
        g0 = starts[c] // group
        lane = lax.broadcasted_iota(jnp.int32, (2, fscale_ref.shape[2]), 1)
        fs_all, ss_all = fscale_out[0], sscale_out[0]
        for i, (m, v) in enumerate(moments):
            cols = pl.ds(starts[c] + i * group, group)
            nfs = jnp.max(jnp.abs(m), axis=1, keepdims=True) + 1e-06
            nss = jnp.max(jnp.abs(v), axis=1, keepdims=True) + 1e-06
            first_out[0, :, cols] = (m / nfs).astype(jnp.bfloat16)
            second_out[0, :, cols] = (v / nss).astype(jnp.bfloat16)
            fs_all = jnp.where(lane == g0 + i, nfs, fs_all)
            ss_all = jnp.where(lane == g0 + i, nss, ss_all)
        fscale_out[0], sscale_out[0] = fs_all, ss_all

    fscale_out[...] = jnp.zeros_like(fscale_out)
    sscale_out[...] = jnp.zeros_like(sscale_out)

    taken = []
    for stage, c in stage_order(n):
        if stage == 0:
            fetch(c).wait()
            if c + 2 < n:
                fetch(c + 2).start()
            res = jnp.dot(lhs[...], act[c][...], preferred_element_type=jnp.float32)
            part[c][...] = res.reshape(part[c].shape)
            pair_copy(c).start()
        elif stage == 1:
            pair_copy(c).wait_recv()
            for j in list(range(1, nq)) + [nq]:
                at = quad_at(j)
                part[c][core, at] = part[c][core, at] + rx1[c][at]
                if j < nq:
                    quad_copy(c, j).start()
        elif stage == 2:
            total = part[c][core, quad]
            for j in range(1, nq):
                quad_copy(c, j).wait_recv()
                total = total + rx2[c][j - 1]
            for g in range(ny):
                s2[c][g] = total[2 * g:2 * g + 2]
            for j in range(1, ny):
                gy_copy(c, j).start()
        elif stage == 3:
            grad = s2[c][gy]
            for j in range(1, ny):
                gy_copy(c, j).wait_recv()
                grad = grad + rx3[c][j - 1]
            if not taken:
                for i in range(2, 7):
                    take(i).wait()
                taken.append(True)
            moments = adam(c, grad)
            for j in range(1, ny):
                ag_copy(c, j).start()
            requant(c, moments)
        elif stage == 4:
            for j in range(1, ny):
                ag_copy(c, j).wait_recv()
            for j in range(1, nq):
                aq_copy(c, j).start()
            ap_copy(c, 0).start()
        elif stage == 5:
            for j in range(1, nq):
                aq_copy(c, j).wait_recv()
                ap_copy(c, j).start()
        else:
            for j in range(nq):
                ap_copy(c, j).wait_recv()

    for c in range(n):
        pair_copy(c).wait_send()
        for j in range(1, nq):
            quad_copy(c, j).wait_send()
            aq_copy(c, j).wait_send()
        for j in range(1, ny):
            gy_copy(c, j).wait_send()
            ag_copy(c, j).wait_send()
        for j in range(nq):
            ap_copy(c, j).wait_send()


def spill(*refs):
    count = (len(refs) - 1) // 2
    sem = refs[-1]
    copies = [
        pltpu.make_async_copy(refs[i], refs[count + i], sem.at[i]) for i in range(count)]
    for copy in copies:
        copy.start()
    for copy in copies:
        copy.wait()


def body(nx, ny, activations, out_grad, master, first_moment, first_scale, second_moment, second_scale):
    tokens, width_all = activations.shape
    rows = out_grad.shape[2]
    group = width_all // first_scale.shape[2]
    widths = chunk_widths(width_all, group)
    n = len(widths)
    nq = nx // 2
    assert rows == nx * ny and nx % 2 == 0

    perm = np.zeros((2, 2 * rows, rows), np.float32)
    spot = 0
    for core in range(2):
        for quad in range(nq):
            for g in range(ny):
                for p in range(2):
                    perm[p, spot, (quad * 2 + core) * ny + g] = 1.0
                    spot += 1
    perm = jnp.asarray(perm, jnp.bfloat16)

    vmem = pl.BlockSpec(memory_space=pltpu.VMEM)
    f32, bf16 = jnp.float32, jnp.bfloat16
    dma = pltpu.SemaphoreType.DMA
    grads = jnp.swapaxes(out_grad, 1, 2)
    small = (grads, perm, master, first_moment, first_scale, second_moment, second_scale)
    scratch = [pltpu.VMEM(x.shape, x.dtype) for x in small] + [dma((len(small),))]
    scratch += [pltpu.VMEM((2 * rows, tokens), bf16)]
    scratch += [pltpu.VMEM((tokens, w), bf16) for w in widths]
    scratch += [pltpu.VMEM((2, nq, 2 * ny, w), f32) for w in widths]
    scratch += [pltpu.VMEM((nq, 2 * ny, w), f32) for w in widths]
    scratch += [pltpu.VMEM((nq - 1, 2 * ny, w), f32) for w in widths]
    scratch += [pltpu.VMEM((ny, 2, w), f32) for w in widths]
    scratch += [pltpu.VMEM((ny - 1, 2, w), f32) for w in widths]
    scratch += [dma((n,)), dma((n,)), dma((n,))]
    scratch += [dma((n, nq - 1)), dma((n, nq - 1)), dma((n, ny - 1)), dma((n, ny - 1))]
    scratch += [dma((n, ny - 1)), dma((n, ny - 1)), dma((n, nq - 1)), dma((n, nq - 1))]
    scratch += [dma((n, nq)), dma((n, nq))]
    held = sum(
        int(np.prod(x.shape)) * jnp.dtype(x.dtype).itemsize
        for x in scratch if x.memory_space == pltpu.VMEM)
    shape = jax.ShapeDtypeStruct
    outs = pl.pallas_call(
        functools.partial(kernel, nx, ny, widths, group),
        out_shape=(
            shape((rows, 2, width_all), bf16),
            shape(master.shape, f32),
            shape(first_moment.shape, bf16),
            shape(first_scale.shape, f32),
            shape(second_moment.shape, bf16),
            shape(second_scale.shape, f32),
        ),
        in_specs=[pl.BlockSpec(memory_space=pltpu.HBM)] * 8,
        out_specs=[vmem] * 6,
        scratch_shapes=scratch,
        compiler_params=pltpu.CompilerParams(
            collective_id=0, has_side_effects=True, vmem_limit_bytes=min(held + held // 8 + 4 * 1024 * 1024, 60 * 1024 * 1024)),
    )(*(pltpu.with_memory_space_constraint(x, pltpu.HBM) for x in (activations, *small)))
    return pl.pallas_call(
        spill,
        out_shape=tuple(shape(out.shape, out.dtype) for out in outs),
        in_specs=[vmem] * 6,
        out_specs=[pl.BlockSpec(memory_space=pltpu.HBM)] * 6,
        scratch_shapes=[dma((6,))],
        compiler_params=pltpu.CompilerParams(vmem_limit_bytes=1024 * 1024),
    )(*outs)


def solution(mesh):
    nx, ny = mesh.shape["gx"], mesh.shape["gy"]
    rows = P(("gx", "gy"), None, None)
    in_specs = (P(("gx", "gy"), None), P(None, ("gx", "gy"), None), rows, rows, rows, rows, rows)
    out_specs = (P(), rows, rows, rows, rows, rows)
    return jax.shard_map(
        functools.partial(body, nx, ny), mesh=mesh, in_specs=in_specs, out_specs=out_specs,
        check_vma=False)
```
